32 devices in a mesh: rows: 16 (over z, x, core), feat: 2 (over y).
Axes of the slice: x: 2, y: 2, z: 4, core: 2. Of those that a mesh axis runs over, the one named last changes fastest.
Arguments:
- train_cells: bfloat16 [1024, 1536], P('rows', 'feat'), may hold values from -24 to 24
- test_cells: bfloat16 [512, 1536], P('rows', 'feat'), may hold values from -24 to 24
- feat_weights: bfloat16 [4, 192, 192], replicated
- row_weights: bfloat16 [4, 192, 192], replicated
- mlp_up: bfloat16 [192, 768], replicated, may hold values from -0.4375 to 0.4375
- mlp_down: bfloat16 [768, 192], replicated, may hold values from -0.21875 to 0.21875
Outputs:
- train_out: bfloat16 [1024, 1536], P('rows', 'feat')
- test_out: bfloat16 [512, 1536], P('rows', 'feat')
The draws below stay inside these ranges and needn't reach their ends.
All inputs are finite; a program needn't handle non-finite values.
Results may differ from the reference program's by a relative error of at most 0.017.
Values may be sent and summed in bfloat16 or wider, within the bound.
A program may use at most 128 MiB of HBM per device.

```python
import math
import jax
import jax.numpy as jnp
from jax import lax

E = 192
HEADS = 6
HD = 32
HID = 768
F = 8
TRAIN = 1024
TEST = 512


def attention_weights(key, query_gain):
    split_keys = jax.random.split(key, 4)
    spread = E ** (-0.5)
    query_w = jax.random.normal(split_keys[0], (E, E), jnp.float32) * query_gain * spread
    key_w = jax.random.normal(split_keys[1], (E, E), jnp.float32) * spread
    value_w = jax.random.normal(split_keys[2], (E, E), jnp.float32) * spread
    output_w = jax.random.normal(split_keys[3], (E, E), jnp.float32) * spread
    return jnp.stack([query_w, key_w, value_w, output_w]).astype(jnp.bfloat16)


def draw_feat_weights(key, part):
    return attention_weights(jax.random.fold_in(key, 3), 1.5)


def draw_row_weights(key, part):
    return attention_weights(jax.random.fold_in(key, 5), 2.5)


def train_table(key):
    key_base = jax.random.fold_in(key, 0)
    table = jax.random.normal(key_base, (TRAIN, F, E), jnp.float32)
    return jnp.clip(table, -24.0, 24.0)


def draw_train_cells(key, part):
    return train_table(jax.random.fold_in(key, 11)).reshape(TRAIN, F * E).astype(jnp.bfloat16)


def draw_test_cells(key, part):
    fresh = jax.random.normal(jax.random.fold_in(key, 13), (TEST, F, E), jnp.float32)
    return jnp.clip(fresh, -24.0, 24.0).reshape(TEST, F * E).astype(jnp.bfloat16)


def bell_draw(key, dims, scale, limit, kind=jnp.bfloat16):
    values = scale * jax.random.normal(key, dims, jnp.float32)
    return jnp.clip(values, min=-limit, max=limit).astype(kind)


def setup_inputs(seed: int = 0) -> dict:
    key_list = jax.random.split(jax.random.key(seed), 7)
    train_cells = draw_train_cells(jax.random.fold_in(key_list[6], 71), 0)
    test_cells = draw_test_cells(jax.random.fold_in(key_list[6], 71), 0)
    feat_weights = draw_feat_weights(jax.random.fold_in(key_list[6], 71), 0)
    row_weights = draw_row_weights(jax.random.fold_in(key_list[6], 71), 0)
    mlp_up = bell_draw(key_list[4], (E, HID), E ** -0.5, 0.4375)
    mlp_down = bell_draw(key_list[5], (HID, E), HID ** -0.5, 0.21875)
    return dict(train_cells=train_cells, test_cells=test_cells, feat_weights=feat_weights, row_weights=row_weights, mlp_up=mlp_up, mlp_down=mlp_down)


eps_norm = 1e-05

def layer_norm(values_in):
    centred = values_in - lax.optimization_barrier(jnp.mean(values_in, axis=-1, keepdims=True))
    spread = lax.optimization_barrier(jnp.mean(centred * centred, axis=-1, keepdims=True))
    return centred * lax.rsqrt(spread + eps_norm)

def project(normed, weight):
    return jnp.dot(normed.reshape(-1, E), weight, preferred_element_type=jnp.float32)

def round_back(values_in):
    return lax.optimization_barrier(values_in.astype(jnp.bfloat16)).astype(jnp.float32)

def feature_attention(queries, key_heads, value_heads):
    scores = jnp.einsum('rqhd,rkhd->rhqk', queries.astype(jnp.float32), key_heads.astype(jnp.float32)) * HD ** (-0.5)
    row_peak = lax.optimization_barrier(jnp.max(scores, axis=-1, keepdims=True))
    weights = jnp.exp(scores - row_peak)
    totals = lax.optimization_barrier(jnp.sum(weights, axis=-1))
    mixture = jnp.einsum('rhqk,rkhd->rqhd', round_back(weights), value_heads.astype(jnp.float32))
    return (mixture / jnp.transpose(totals, (0, 2, 1))[..., None]).astype(jnp.bfloat16)

def row_attention(queries, key_heads, value_heads):
    total_rows = queries.shape[0]
    block_rows = math.gcd(total_rows, 1024)
    query_feat = jnp.transpose(queries, (1, 0, 2, 3)).reshape(F, total_rows // block_rows, block_rows, HEADS, HD)
    key_feat = jnp.transpose(key_heads, (1, 0, 2, 3))
    value_feat = jnp.transpose(value_heads, (1, 0, 2, 3))

    def one_feature(inputs):
        query_blocks, key_one, value_one = inputs
        key_float = key_one.astype(jnp.float32)
        value_float = value_one.astype(jnp.float32)

        def one_block(query_block):
            scores = jnp.einsum('qhd,khd->hqk', query_block.astype(jnp.float32), key_float) * HD ** (-0.5)
            row_peak = lax.optimization_barrier(jnp.max(scores, axis=-1, keepdims=True))
            weights = jnp.exp(scores - row_peak)
            totals = lax.optimization_barrier(jnp.sum(weights, axis=-1))
            mixture = jnp.einsum('hqk,khd->qhd', round_back(weights), value_float)
            return (mixture / jnp.transpose(totals)[..., None]).astype(jnp.bfloat16)
        return lax.map(one_block, query_blocks).reshape(total_rows, HEADS, HD)
    mixture = lax.map(one_feature, (query_feat, key_feat, value_feat))
    return jnp.transpose(mixture, (1, 0, 2, 3))

def reference(train_cells, test_cells, feat_weights, row_weights, mlp_up, mlp_down):
    joined = jnp.concatenate([train_cells, test_cells], axis=0)
    height = joined.shape[0]
    start_cells = joined.astype(jnp.float32).reshape(height, F, E)
    normed_one = layer_norm(start_cells).astype(jnp.bfloat16)
    feat_query = project(normed_one, feat_weights[0]).astype(jnp.bfloat16).reshape(height, F, HEADS, HD)
    feat_key = project(normed_one, feat_weights[1]).astype(jnp.bfloat16).reshape(height, F, HEADS, HD)
    feat_value = project(normed_one, feat_weights[2]).astype(jnp.bfloat16).reshape(height, F, HEADS, HD)
    feat_mix = feature_attention(feat_query, feat_key, feat_value)
    feat_out = project(feat_mix, feat_weights[3]).astype(jnp.bfloat16).reshape(height, F, E)
    after_feat = start_cells + feat_out.astype(jnp.float32)
    normed_two = layer_norm(after_feat).astype(jnp.bfloat16)
    row_query = project(normed_two, row_weights[0]).astype(jnp.bfloat16).reshape(height, F, HEADS, HD)
    train_normed = normed_two[:TRAIN]
    row_key = project(train_normed, row_weights[1]).astype(jnp.bfloat16).reshape(TRAIN, F, HEADS, HD)
    row_value = project(train_normed, row_weights[2]).astype(jnp.bfloat16).reshape(TRAIN, F, HEADS, HD)
    row_mix = row_attention(row_query, row_key, row_value)
    after_row = after_feat + project(row_mix, row_weights[3]).reshape(height, F, E)
    normed_three = layer_norm(after_row).astype(jnp.bfloat16)
    hidden = jax.nn.gelu(jnp.dot(normed_three.reshape(-1, E), mlp_up, preferred_element_type=jnp.float32), approximate=False).astype(jnp.bfloat16)
    lowered = jnp.dot(hidden, mlp_down, preferred_element_type=jnp.float32).reshape(height, F, E)
    result = (after_row + lowered).astype(jnp.bfloat16).reshape(height, F * E)
    return (result[:TRAIN], result[TRAIN:])
```

```python
import functools

import jax
import jax.numpy as jnp
from jax import lax
from jax.experimental import pallas as pl
from jax.experimental.pallas import tpu as pltpu
from jax.sharding import PartitionSpec as P

HD = 32
EPS = 1e-05
LOG2E = 1.4426950408889634
MESH = pl.DeviceIdType.MESH
BF = jnp.bfloat16
F32 = jnp.float32


def layer_norm(x):
    centred = x - jnp.mean(x, axis=-1, keepdims=True)
    spread = jnp.mean(centred * centred, axis=-1, keepdims=True)
    return centred * lax.rsqrt(spread + EPS)


def dot(a, b):
    return jnp.dot(a, b, preferred_element_type=F32)


def dot_t(a, b):
    return lax.dot_general(a, b, (((1,), (1,)), ((), ())), preferred_element_type=F32)


def pack(x):
    n = x.shape[0]
    low = jnp.concatenate([x[: n // 2, 128:], x[n // 2 :, 128:]], axis=1)
    return jnp.concatenate([x[:, :128], low], axis=0)


def unpack(p):
    n = p.shape[0] * 2 // 3
    low = p[n:]
    high = jnp.concatenate([low[:, :64], low[:, 64:]], axis=0)
    return jnp.concatenate([p[:n], high], axis=1)


def gelu(x):
    return 0.5 * x * (1.0 + lax.erf(x * (0.5**0.5)))


def kernel(
    rows_n,
    feats_n,
    train_ref,
    test_ref,
    fw_hbm,
    rw_hbm,
    up_hbm,
    down_hbm,
    train_out,
    test_out,
    fw,
    rw,
    up,
    down,
    o_train,
    o_test,
    outbox,
    inbox,
    ring,
    scores,
    values,
    queries,
    back_out,
    back_in,
    w_sem,
    f_send,
    f_recv,
    q_send,
    q_recv,
    r_send,
    r_recv,
    b_send,
    b_recv,
):
    width = fw.shape[-1]
    quad = outbox.shape[0]
    heads = width // HD
    groups_n = rows_n // quad
    half = groups_n // 2
    n_train = train_ref.shape[0]
    n_test = test_ref.shape[0]
    cell_rows = n_train + n_test
    scale = LOG2E * HD ** (-0.5)

    my_row = lax.axis_index("rows")
    my_feat = lax.axis_index("feat")
    member = lax.rem(my_row, quad)
    group = my_row // quad

    def mate(k):
        return group * quad + lax.rem(member + k, quad)

    right = lax.rem(group + 1, groups_n) * quad + member
    left = lax.rem(group + groups_n - 1, groups_n) * quad + member
    other = lax.rem(my_feat + 1, feats_n)

    loads = [
        pltpu.make_async_copy(s, d, w_sem.at[i])
        for i, (s, d) in enumerate([(fw_hbm, fw), (rw_hbm, rw), (up_hbm, up), (down_hbm, down)])
    ]
    for c in loads:
        c.start()

    barrier = pltpu.get_barrier_semaphore()
    pl.semaphore_signal(barrier, inc=1, device_id={"feat": other}, device_id_type=MESH)
    for k in range(1, quad):
        pl.semaphore_signal(barrier, inc=1, device_id={"rows": mate(k)}, device_id_type=MESH)
    for d in (right, left):
        pl.semaphore_signal(barrier, inc=1, device_id={"rows": d}, device_id_type=MESH)
    pl.semaphore_wait(barrier, quad + 2)

    swaps = [
        pltpu.make_async_remote_copy(
            src_ref=s,
            dst_ref=d,
            send_sem=f_send.at[i],
            recv_sem=f_recv.at[i],
            device_id={"feat": other},
            device_id_type=MESH,
        )
        for i, (s, d) in enumerate([(train_ref, o_train), (test_ref, o_test)])
    ]
    for c in swaps:
        c.start()

    def feature_rows(tr, te):
        parts = []
        for f in range(quad):
            sl = slice(f * width, (f + 1) * width)
            parts += [tr[:, sl].astype(F32), te[:, sl].astype(F32)]
        return jnp.concatenate(parts, axis=0)

    def split(x):
        return [x[f * cell_rows : (f + 1) * cell_rows] for f in range(quad)]

    cells = feature_rows(train_ref[...], test_ref[...])
    n_one = layer_norm(cells).astype(BF)
    loads[0].wait()
    q = split((dot(n_one, fw[0]) * scale).astype(BF))
    ks = split(dot(n_one, fw[1]).astype(BF))
    vs = split(dot(n_one, fw[2]).astype(BF))
    for c in swaps:
        c.wait()
    n_two = layer_norm(feature_rows(o_train[...], o_test[...])).astype(BF)
    ks += split(dot(n_two, fw[1]).astype(BF))
    vs += split(dot(n_two, fw[2]).astype(BF))

    same = (
        lax.broadcasted_iota(jnp.int32, (width, width), 0) // HD
        == lax.broadcasted_iota(jnp.int32, (width, width), 1) // HD
    )
    spread = jnp.where(same, 1.0, 0.0).astype(BF)
    mixes = []
    for f in range(quad):
        prod = jnp.concatenate([q[f] * k for k in ks], axis=0)
        s = dot(prod, spread)
        s = [s[g * cell_rows : (g + 1) * cell_rows] for g in range(len(ks))]
        top = functools.reduce(jnp.maximum, s)
        total = None
        mix = None
        for g in range(len(ks)):
            e = jnp.exp2(s[g] - top)
            t = e * vs[g].astype(F32)
            total = e if total is None else total + e
            mix = t if mix is None else mix + t
        mixes.append((mix / total).astype(BF))
    feat_out = dot(jnp.concatenate(mixes, axis=0), fw[3])
    after = split((cells + feat_out).astype(BF))
    for f in range(quad):
        outbox[f] = pack(after[f])

    sends = []
    for k in (2, 3, 1):
        c = pltpu.make_async_remote_copy(
            src_ref=outbox.at[lax.rem(member + k, quad)],
            dst_ref=inbox.at[k],
            send_sem=q_send.at[k],
            recv_sem=q_recv.at[k],
            device_id={"rows": mate(k)},
            device_id_type=MESH,
        )
        c.start()
        sends.append(c)
    inbox[0] = outbox[member]
    for c in sends:
        c.wait()

    after_feat = [unpack(inbox[k]).astype(F32) for k in range(quad)]
    normed = [layer_norm(x).astype(BF) for x in after_feat]
    for p in range(2):
        ring[0, p] = pack(
            jnp.concatenate([normed[2 * p][:n_train], normed[2 * p + 1][:n_train]], axis=0)
        )

    def hop(way, h, p):
        last = h == half - 1
        src = 0 if h == 0 else 2 * h - 1 + way
        dst = 2 * half - 1 if last else 1 + 2 * h + way
        return pltpu.make_async_remote_copy(
            src_ref=ring.at[src, p],
            dst_ref=ring.at[dst, p],
            send_sem=r_send.at[way, h, p],
            recv_sem=r_recv.at[way, h, p],
            device_id={"rows": left if way else right},
            device_id_type=MESH,
        )

    def pieces(way, h):
        return (way,) if h == half - 1 else (way, 1 - way)

    hops = {}
    for way in range(2):
        for p in pieces(way, 0):
            hops[way, 0, p] = hop(way, 0, p)
            hops[way, 0, p].start()

    loads[1].wait()
    n_all = jnp.concatenate(normed, axis=0)
    q_all = (dot(n_all, rw[0]) * scale).astype(BF)
    lane_head = lax.broadcasted_iota(jnp.int32, (1, width), 1) // HD
    for h in range(heads):
        queries[h] = jnp.where(lane_head == h, q_all, jnp.zeros_like(q_all))

    n_query = q_all.shape[0]
    span = 2 * ring.shape[2] * 2 // 3

    def keys_of(slot):
        return jnp.concatenate([unpack(ring[slot, 0]), unpack(ring[slot, 1])], axis=0)

    def take(slot, column):
        x = keys_of(slot)
        key = dot(x, rw[1]).astype(BF)
        value = dot(x, rw[2]).astype(BF)
        rows = slice(column * span, (column + 1) * span)
        values[rows, :width] = value
        for h in range(heads):
            scores[h, :, rows] = dot_t(queries[h], key)

    take(0, 0) if half <= 2 else None
    for h in range(half):
        if h + 1 < half:
            for way in range(2):
                for p in pieces(way, h + 1):
                    hops[way, h, p].wait_recv()
                    hops[way, h + 1, p] = hop(way, h + 1, p)
                    hops[way, h + 1, p].start()
            for way in range(2):
                for p in pieces(way, h):
                    if p not in pieces(way, h + 1):
                        hops[way, h, p].wait_recv()
            if half <= 2:
                take(1 + 2 * h, 1 + 2 * h)
                take(2 + 2 * h, 2 + 2 * h)
        else:
            for way in range(2):
                for p in pieces(way, h):
                    hops[way, h, p].wait_recv()
            if half <= 2:
                take(2 * half - 1, 2 * half - 1)

    values[:, width:] = jnp.ones_like(values[:, width:])

    def attend(h, carried):
        s = scores[h]
        top = jnp.max(s, axis=-1, keepdims=True)
        if carried is not None:
            top = jnp.maximum(top, carried[0])
        e = jnp.exp2(s - top).astype(BF)
        out = dot(e, values[...])
        if carried is not None:
            out = out + carried[1] * jnp.exp2(carried[0] - top)
        return top, out

    if half <= 2:
        states = [attend(h, None) for h in range(heads)]
    else:
        per = scores.shape[2] // span

        def step(i, states):
            for j in range(per):
                take(i * per + j, j)
            return [attend(h, states[h]) for h in range(heads)]

        start = [
            (
                jnp.full((n_query, 1), -1e30, F32),
                jnp.zeros((n_query, values.shape[1]), F32),
            )
            for _ in range(heads)
        ]
        states = lax.fori_loop(0, groups_n // per, step, start)

    mixed = None
    for h in range(heads):
        out = states[h][1]
        part = out[:, :width] * (1.0 / out[:, width : width + 1])
        mixed = part if h == 0 else jnp.where(lane_head == h, part, mixed)
    mixed = mixed.astype(BF)

    for c in loads[2:]:
        c.wait()
    returns = []
    for k in (2, 1, 3, 0):
        rows = slice(k * cell_rows, (k + 1) * cell_rows)
        after_row = after_feat[k] + dot(mixed[rows], rw[3])
        hidden = gelu(dot(layer_norm(after_row).astype(BF), up[...])).astype(BF)
        done = pack((after_row + dot(hidden, down[...])).astype(BF))
        if k == 0:
            back_in[0] = done
            continue
        back_out[k] = done
        c = pltpu.make_async_remote_copy(
            src_ref=back_out.at[k],
            dst_ref=back_in.at[k],
            send_sem=b_send.at[k],
            recv_sem=b_recv.at[k],
            device_id={"rows": mate(quad - k)},
            device_id_type=MESH,
        )
        c.start()
        returns.append(c)
    for c in returns:
        c.wait()
    for c in hops.values():
        c.wait_send()

    outs = [unpack(back_in[lax.rem(f + quad - member, quad)]) for f in range(quad)]
    result = jnp.concatenate(outs, axis=1)
    train_out[...] = result[:n_train]
    test_out[...] = result[n_train:]


def solution(mesh):
    rows_n = mesh.shape["rows"]
    feats_n = mesh.shape["feat"]

    def body(train, test, fw, rw, up, down):
        width = fw.shape[-1]
        quad = train.shape[1] // width
        heads = width // HD
        n_train, n_test = train.shape[0], test.shape[0]
        cell_rows = n_train + n_test
        groups_n = rows_n // quad
        half = groups_n // 2
        span = quad * n_train
        keys = min(groups_n, 4) * span
        packed = cell_rows * width // 128
        vmem = pltpu.VMEM
        dma = pltpu.SemaphoreType.DMA
        vspec = pl.BlockSpec(memory_space=pltpu.VMEM)
        aspec = pl.BlockSpec(memory_space=pl.ANY)
        return pl.pallas_call(
            functools.partial(kernel, rows_n, feats_n),
            out_shape=(
                jax.ShapeDtypeStruct(train.shape, BF),
                jax.ShapeDtypeStruct(test.shape, BF),
            ),
            in_specs=[vspec, vspec, aspec, aspec, aspec, aspec],
            out_specs=(vspec, vspec),
            scratch_shapes=[
                vmem(fw.shape, BF),
                vmem(rw.shape, BF),
                vmem(up.shape, BF),
                vmem(down.shape, BF),
                vmem(train.shape, BF),
                vmem(test.shape, BF),
                vmem((quad, packed, 128), BF),
                vmem((quad, packed, 128), BF),
                vmem((groups_n, 2, span * width // 256, 128), BF),
                vmem((heads, quad * cell_rows, keys), F32),
                vmem((keys, 256), BF),
                vmem((heads, quad * cell_rows, width), BF),
                vmem((quad, packed, 128), BF),
                vmem((quad, packed, 128), BF),
                dma((4,)),
                dma((2,)),
                dma((2,)),
                dma((quad,)),
                dma((quad,)),
                dma((2, half, 2)),
                dma((2, half, 2)),
                dma((quad,)),
                dma((quad,)),
            ],
            compiler_params=pltpu.CompilerParams(
                collective_id=0, has_side_effects=True, vmem_limit_bytes=60 * 1024 * 1024
            ),
            name="layer",
        )(train, test, fw, rw, up, down)

    return jax.shard_map(
        body,
        mesh=mesh,
        in_specs=(P("rows", "feat"), P("rows", "feat"), P(), P(), P(), P()),
        out_specs=(P("rows", "feat"), P("rows", "feat")),
        check_vma=False,
    )
```

```python
import functools

import jax
import jax.numpy as jnp
from jax import lax
from jax.experimental import pallas as pl
from jax.experimental.pallas import tpu as pltpu
from jax.sharding import PartitionSpec as P

HD = 32
EPS = 1e-05
LOG2E = 1.4426950408889634
MESH = pl.DeviceIdType.MESH
BF = jnp.bfloat16
F32 = jnp.float32


def layer_norm(x):
    centred = x - jnp.mean(x, axis=-1, keepdims=True)
    spread = jnp.mean(centred * centred, axis=-1, keepdims=True)
    return centred * lax.rsqrt(spread + EPS)


def dot(a, b):
    return jnp.dot(a, b, preferred_element_type=F32)


def dot_t(a, b):
    return lax.dot_general(a, b, (((1,), (1,)), ((), ())), preferred_element_type=F32)


def pack(x):
    n = x.shape[0]
    low = jnp.concatenate([x[: n // 2, 128:], x[n // 2 :, 128:]], axis=1)
    return jnp.concatenate([x[:, :128], low], axis=0)


def unpack(p):
    n = p.shape[0] * 2 // 3
    low = p[n:]
    high = jnp.concatenate([low[:, :64], low[:, 64:]], axis=0)
    return jnp.concatenate([p[:n], high], axis=1)


def gelu(x):
    return 0.5 * x * (1.0 + lax.erf(x * (0.5**0.5)))


def kernel(
    rows_n,
    feats_n,
    train_hbm,
    test_hbm,
    fw_hbm,
    rw_hbm,
    up_hbm,
    down_hbm,
    train_out,
    test_out,
    fw,
    rw,
    up,
    down,
    train_ref,
    test_ref,
    o_train,
    o_test,
    outbox,
    inbox,
    t_outbox,
    t_inbox,
    ring,
    scores,
    values,
    queries,
    back_out,
    back_in,
    w_sem,
    f_send,
    f_recv,
    q_send,
    q_recv,
    t_send,
    t_recv,
    r_send,
    r_recv,
    b_send,
    b_recv,
):
    width = fw.shape[-1]
    quad = outbox.shape[0]
    heads = width // HD
    groups_n = rows_n // quad
    half = groups_n // 2
    n_train = train_ref.shape[0]
    n_test = test_ref.shape[0]
    scale = LOG2E * HD ** (-0.5)

    my_row = lax.axis_index("rows")
    my_feat = lax.axis_index("feat")
    member = lax.rem(my_row, quad)
    group = my_row // quad

    def partner(k):
        low, high = lax.rem(member, 2), member // 2
        return (1 - high if k // 2 else high) * 2 + (1 - low if k % 2 else low)

    def mate(k):
        return group * quad + partner(k)

    right = lax.rem(group + 1, groups_n) * quad + member
    left = lax.rem(group + groups_n - 1, groups_n) * quad + member
    other = lax.rem(my_feat + 1, feats_n)

    loads = [
        pltpu.make_async_copy(s, d, w_sem.at[i])
        for i, (s, d) in enumerate(
            [
                (train_hbm, train_ref),
                (fw_hbm, fw),
                (test_hbm, test_ref),
                (rw_hbm, rw),
                (up_hbm, up),
                (down_hbm, down),
            ]
        )
    ]
    for c in loads:
        c.start()

    barrier = pltpu.get_barrier_semaphore()
    pl.semaphore_signal(barrier, inc=1, device_id={"feat": other}, device_id_type=MESH)
    for k in range(1, quad):
        pl.semaphore_signal(barrier, inc=1, device_id={"rows": mate(k)}, device_id_type=MESH)
    for d in (right, left):
        pl.semaphore_signal(barrier, inc=1, device_id={"rows": d}, device_id_type=MESH)
    pl.semaphore_wait(barrier, quad + 2)

    swaps = [
        pltpu.make_async_remote_copy(
            src_ref=s,
            dst_ref=d,
            send_sem=f_send.at[i],
            recv_sem=f_recv.at[i],
            device_id={"feat": other},
            device_id_type=MESH,
        )
        for i, (s, d) in enumerate([(train_hbm, o_train), (test_hbm, o_test)])
    ]
    for c in swaps:
        c.start()

    def feature_rows(table):
        return jnp.concatenate(
            [table[:, f * width : (f + 1) * width].astype(F32) for f in range(quad)], axis=0
        )

    def split(x):
        n = x.shape[0] // quad
        return [x[f * n : (f + 1) * n] for f in range(quad)]

    def key_value(normed):
        return split(dot(normed, fw[1]).astype(BF)), split(dot(normed, fw[2]).astype(BF))

    same = (
        lax.broadcasted_iota(jnp.int32, (width, width), 0) // HD
        == lax.broadcasted_iota(jnp.int32, (width, width), 1) // HD
    )
    spread = jnp.where(same, 1.0, 0.0).astype(BF)

    def own_side(table):
        cells = feature_rows(table)
        normed = layer_norm(cells).astype(BF)
        q = split((dot(normed, fw[0]) * scale).astype(BF))
        ks, vs = key_value(normed)
        return cells, q, ks, vs

    def feature_attention(own, table):
        cells, q, ks, vs = own
        n = table.shape[0]
        more_k, more_v = key_value(layer_norm(feature_rows(table)).astype(BF))
        ks, vs = ks + more_k, vs + more_v
        mixes = []
        for f in range(quad):
            prod = jnp.concatenate([q[f] * k for k in ks], axis=0)
            s = dot(prod, spread)
            s = [s[g * n : (g + 1) * n] for g in range(len(ks))]
            top = functools.reduce(jnp.maximum, s)
            total = None
            mix = None
            for g in range(len(ks)):
                e = jnp.exp2(s[g] - top)
                t = e * vs[g].astype(F32)
                total = e if total is None else total + e
                mix = t if mix is None else mix + t
            mixes.append((mix / total).astype(BF))
        feat_out = dot(jnp.concatenate(mixes, axis=0), fw[3])
        return split((cells + feat_out).astype(BF))

    def to_mates(box, landing, send, recv):
        copies = {}
        for k in (2, 3, 1):
            copies[k] = pltpu.make_async_remote_copy(
                src_ref=box.at[partner(k)],
                dst_ref=landing.at[k],
                send_sem=send.at[k],
                recv_sem=recv.at[k],
                device_id={"rows": mate(k)},
                device_id_type=MESH,
            )
            copies[k].start()
        landing[0] = box[member]
        return copies

    loads[0].wait()
    loads[1].wait()
    own = own_side(train_ref[...])
    loads[2].wait()
    own_test = own_side(test_ref[...])
    swaps[0].wait()
    for f, x in enumerate(feature_attention(own, o_train[...])):
        outbox[f] = pack(x)
    moved = to_mates(outbox, inbox, q_send, q_recv)

    def hop(way, h, p):
        last = h == half - 1
        src = 0 if h == 0 else 2 * h - 1 + way
        dst = 2 * half - 1 if last else 1 + 2 * h + way
        return pltpu.make_async_remote_copy(
            src_ref=ring.at[src, p],
            dst_ref=ring.at[dst, p],
            send_sem=r_send.at[way, h, p],
            recv_sem=r_recv.at[way, h, p],
            device_id={"rows": left if way else right},
            device_id_type=MESH,
        )

    def pieces(way, h):
        return (way,) if h == half - 1 else (way, 1 - way)

    hops = {}
    after_train = []
    normed_train = []
    for p in range(2):
        for k in (2 * p, 2 * p + 1):
            if k:
                moved[k].wait_recv()
            after_train.append(unpack(inbox[k]).astype(F32))
            normed_train.append(layer_norm(after_train[k]).astype(BF))
        ring[0, p] = pack(jnp.concatenate(normed_train[2 * p :], axis=0))
        for way in (p, 1 - p):
            if p in pieces(way, 0):
                hops[way, 0, p] = hop(way, 0, p)
                hops[way, 0, p].start()

    swaps[1].wait()
    for f, x in enumerate(feature_attention(own_test, o_test[...])):
        t_outbox[f] = pack(x)
    t_moved = to_mates(t_outbox, t_inbox, t_send, t_recv)

    loads[3].wait()
    lane_head = lax.broadcasted_iota(jnp.int32, (1, width), 1) // HD
    train_rows = slice(0, quad * n_train)
    test_rows = slice(quad * n_train, quad * (n_train + n_test))
    all_rows = slice(0, quad * (n_train + n_test))
    n_query = all_rows.stop
    span = quad * n_train
    values[:, width:] = jnp.ones_like(values[:, width:])

    def ask(normed, rows):
        q_all = (dot(jnp.concatenate(normed, axis=0), rw[0]) * scale).astype(BF)
        for h in range(heads):
            queries[h, rows] = jnp.where(lane_head == h, q_all, jnp.zeros_like(q_all))

    def take(slot, column):
        x = jnp.concatenate([unpack(ring[slot, 0]), unpack(ring[slot, 1])], axis=0)
        values[column * span : (column + 1) * span, :width] = dot(x, rw[2]).astype(BF)
        return dot(x, rw[1]).astype(BF)

    def score(key, column, rows):
        for h in range(heads):
            scores[h, rows, column * span : (column + 1) * span] = dot_t(queries[h, rows], key)

    def attend(h, columns, carried):
        s = scores[h, :, columns]
        top = jnp.max(s, axis=-1, keepdims=True)
        if carried is not None:
            top = jnp.maximum(top, carried[0])
        e = jnp.exp2(s - top).astype(BF)
        out = dot(e, values[columns])
        if carried is not None:
            out = out + carried[1] * jnp.exp2(carried[0] - top)
        return top, out

    ask(normed_train, train_rows)
    if half <= 2:
        own_key = take(0, 0)
        score(own_key, 0, train_rows)

    for h in range(half - 1):
        for way in range(2):
            for p in pieces(way, h + 1):
                hops[way, h, p].wait_recv()
                hops[way, h + 1, p] = hop(way, h + 1, p)
                hops[way, h + 1, p].start()
        for way in range(2):
            for p in pieces(way, h):
                if p not in pieces(way, h + 1):
                    hops[way, h, p].wait_recv()

    after_test = []
    normed_test = []
    for k in range(quad):
        if k:
            t_moved[k].wait_recv()
        after_test.append(unpack(t_inbox[k]).astype(F32))
        normed_test.append(layer_norm(after_test[k]).astype(BF))
    ask(normed_test, test_rows)

    if half <= 2:
        score(own_key, 0, test_rows)
        for slot in range(1, 2 * half - 1):
            score(take(slot, slot), slot, all_rows)
        last = 2 * half - 1
        states = [attend(h, slice(0, last * span), None) for h in range(heads)]

    for way in range(2):
        for p in pieces(way, half - 1):
            hops[way, half - 1, p].wait_recv()

    if half <= 2:
        score(take(last, last), last, all_rows)
        columns = slice(last * span, (last + 1) * span)
        states = [attend(h, columns, states[h]) for h in range(heads)]
    else:
        per = scores.shape[2] // span

        def step(i, states):
            for j in range(per):
                score(take(i * per + j, j), j, all_rows)
            return [attend(h, slice(0, per * span), states[h]) for h in range(heads)]

        start = [
            (
                jnp.full((n_query, 1), -1e30, F32),
                jnp.zeros((n_query, values.shape[1]), F32),
            )
            for _ in range(heads)
        ]
        states = lax.fori_loop(0, groups_n // per, step, start)

    mixed = None
    for h in range(heads):
        out = states[h][1]
        part = out[:, :width] * (1.0 / out[:, width : width + 1])
        mixed = part if h == 0 else jnp.where(lane_head == h, part, mixed)
    mixed = mixed.astype(BF)

    for c in loads[4:]:
        c.wait()
    returns = []
    for pair in ((2, 3), (1, 0)):
        before, picked = [], []
        for k in pair:
            before += [after_train[k], after_test[k]]
            base = test_rows.start + k * n_test
            picked += [mixed[k * n_train : (k + 1) * n_train], mixed[base : base + n_test]]
        after_row = jnp.concatenate(before, axis=0) + dot(jnp.concatenate(picked, axis=0), rw[3])
        hidden = gelu(dot(layer_norm(after_row).astype(BF), up[...])).astype(BF)
        done = (after_row + dot_t(hidden, down[...])).astype(BF)
        for i, k in enumerate(pair):
            n = n_train + n_test
            block = pack(done[i * n : (i + 1) * n])
            if k == 0:
                back_in[0] = block
                continue
            back_out[k] = block
            c = pltpu.make_async_remote_copy(
                src_ref=back_out.at[k],
                dst_ref=back_in.at[k],
                send_sem=b_send.at[k],
                recv_sem=b_recv.at[k],
                device_id={"rows": mate(k)},
                device_id_type=MESH,
            )
            c.start()
            returns.append(c)
    for c in returns:
        c.wait()
    for c in [*hops.values(), *moved.values(), *t_moved.values()]:
        c.wait_send()

    outs = [unpack(back_in[partner(f)]) for f in range(quad)]
    result = jnp.concatenate(outs, axis=1)
    train_out[...] = result[:n_train]
    test_out[...] = result[n_train:]


def solution(mesh):
    rows_n = mesh.shape["rows"]
    feats_n = mesh.shape["feat"]

    def body(train, test, fw, rw, up, down):
        width = fw.shape[-1]
        quad = train.shape[1] // width
        heads = width // HD
        n_train, n_test = train.shape[0], test.shape[0]
        cell_rows = n_train + n_test
        groups_n = rows_n // quad
        half = groups_n // 2
        span = quad * n_train
        keys = min(groups_n, 4) * span
        packed = cell_rows * width // 128
        vmem = pltpu.VMEM
        dma = pltpu.SemaphoreType.DMA
        vspec = pl.BlockSpec(memory_space=pltpu.VMEM)
        aspec = pl.BlockSpec(memory_space=pl.ANY)
        return pl.pallas_call(
            functools.partial(kernel, rows_n, feats_n),
            out_shape=(
                jax.ShapeDtypeStruct(train.shape, BF),
                jax.ShapeDtypeStruct(test.shape, BF),
            ),
            in_specs=[aspec, aspec, aspec, aspec, aspec, aspec],
            out_specs=(vspec, vspec),
            scratch_shapes=[
                vmem(fw.shape, BF),
                vmem(rw.shape, BF),
                vmem(up.shape, BF),
                vmem(down.shape[::-1], BF),
                vmem(train.shape, BF),
                vmem(test.shape, BF),
                vmem(train.shape, BF),
                vmem(test.shape, BF),
                vmem((quad, n_train * width // 128, 128), BF),
                vmem((quad, n_train * width // 128, 128), BF),
                vmem((quad, n_test * width // 128, 128), BF),
                vmem((quad, n_test * width // 128, 128), BF),
                vmem((groups_n, 2, span * width // 256, 128), BF),
                vmem((heads, quad * cell_rows, keys), F32),
                vmem((keys, 256), BF),
                vmem((heads, quad * cell_rows, width), BF),
                vmem((quad, packed, 128), BF),
                vmem((quad, packed, 128), BF),
                dma((6,)),
                dma((2,)),
                dma((2,)),
                dma((quad,)),
                dma((quad,)),
                dma((quad,)),
                dma((quad,)),
                dma((2, half, 2)),
                dma((2, half, 2)),
                dma((quad,)),
                dma((quad,)),
            ],
            compiler_params=pltpu.CompilerParams(
                collective_id=0, has_side_effects=True, vmem_limit_bytes=60 * 1024 * 1024
            ),
            name="layer",
        )(train, test, fw, rw, up, down.T)

    return jax.shard_map(
        body,
        mesh=mesh,
        in_specs=(P("rows", "feat"), P("rows", "feat"), P(), P(), P(), P()),
        out_specs=(P("rows", "feat"), P("rows", "feat")),
        check_vma=False,
    )
```

```python
import functools

import jax
import jax.numpy as jnp
from jax import lax
from jax.experimental import pallas as pl
from jax.experimental.pallas import tpu as pltpu
from jax.sharding import PartitionSpec as P

HD = 32
EPS = 1e-05
LOG2E = 1.4426950408889634
MESH = pl.DeviceIdType.MESH
BF = jnp.bfloat16
F32 = jnp.float32


def layer_norm(x):
    centred = x - jnp.mean(x, axis=-1, keepdims=True)
    spread = jnp.mean(centred * centred, axis=-1, keepdims=True)
    return centred * lax.rsqrt(spread + EPS)


def dot(a, b):
    return jnp.dot(a, b, preferred_element_type=F32)


def dot_t(a, b):
    return lax.dot_general(a, b, (((1,), (1,)), ((), ())), preferred_element_type=F32)


def pack(x):
    n = x.shape[0]
    low = jnp.concatenate([x[: n // 2, 128:], x[n // 2 :, 128:]], axis=1)
    return jnp.concatenate([x[:, :128], low], axis=0)


def unpack(p):
    n = p.shape[0] * 2 // 3
    low = p[n:]
    high = jnp.concatenate([low[:, :64], low[:, 64:]], axis=0)
    return jnp.concatenate([p[:n], high], axis=1)


def gelu(x):
    return 0.5 * x * (1.0 + lax.erf(x * (0.5**0.5)))


def kernel(
    rows_n,
    feats_n,
    train_hbm,
    test_hbm,
    fw_hbm,
    rw_hbm,
    up_hbm,
    down_hbm,
    back_in,
    fw,
    rw,
    up,
    down,
    train_ref,
    test_ref,
    o_train,
    o_test,
    outbox,
    inbox,
    t_outbox,
    t_inbox,
    ring,
    scores,
    values,
    queries,
    back_out,
    w_sem,
    f_send,
    f_recv,
    q_send,
    q_recv,
    r_send,
    r_recv,
    b_send,
    b_recv,
):
    width = fw.shape[-1]
    quad = t_outbox.shape[0]
    heads = width // HD
    groups_n = rows_n // quad
    half = groups_n // 2
    n_train = train_ref.shape[0]
    n_test = test_ref.shape[0]
    n_half = n_train // 2
    scale = LOG2E * HD ** (-0.5)

    my_row = lax.axis_index("rows")
    my_feat = lax.axis_index("feat")
    member = lax.rem(my_row, quad)
    group = my_row // quad

    def partner(k):
        low, high = lax.rem(member, 2), member // 2
        return (1 - high if k // 2 else high) * 2 + (1 - low if k % 2 else low)

    def mate(k):
        return group * quad + partner(k)

    right = lax.rem(group + 1, groups_n) * quad + member
    left = lax.rem(group + groups_n - 1, groups_n) * quad + member
    other = lax.rem(my_feat + 1, feats_n)

    loads = [
        pltpu.make_async_copy(s, d, w_sem.at[i])
        for i, (s, d) in enumerate(
            [
                (train_hbm, train_ref),
                (fw_hbm, fw),
                (test_hbm, test_ref),
                (rw_hbm, rw),
                (up_hbm, up),
                (down_hbm, down),
            ]
        )
    ]
    for c in loads:
        c.start()

    barrier = pltpu.get_barrier_semaphore()
    pl.semaphore_signal(barrier, inc=1, device_id={"feat": other}, device_id_type=MESH)
    for k in range(1, quad):
        pl.semaphore_signal(barrier, inc=1, device_id={"rows": mate(k)}, device_id_type=MESH)
    for d in (right, left):
        pl.semaphore_signal(barrier, inc=1, device_id={"rows": d}, device_id_type=MESH)
    pl.semaphore_wait(barrier, quad + 2)

    halves = [pl.ds(p * n_half, n_half) for p in range(2)]
    swaps = [
        pltpu.make_async_remote_copy(
            src_ref=s,
            dst_ref=d,
            send_sem=f_send.at[i],
            recv_sem=f_recv.at[i],
            device_id={"feat": other},
            device_id_type=MESH,
        )
        for i, (s, d) in enumerate(
            [(train_hbm.at[r], o_train.at[r]) for r in halves] + [(test_hbm, o_test)]
        )
    ]
    for c in swaps:
        c.start()

    def feature_rows(table):
        return jnp.concatenate(
            [table[:, f * width : (f + 1) * width].astype(F32) for f in range(quad)], axis=0
        )

    def split(x):
        n = x.shape[0] // quad
        return [x[f * n : (f + 1) * n] for f in range(quad)]

    def key_value(normed):
        return split(dot(normed, fw[1]).astype(BF)), split(dot(normed, fw[2]).astype(BF))

    same = (
        lax.broadcasted_iota(jnp.int32, (width, width), 0) // HD
        == lax.broadcasted_iota(jnp.int32, (width, width), 1) // HD
    )
    spread = jnp.where(same, 1.0, 0.0).astype(BF)

    def own_side(table):
        cells = feature_rows(table)
        normed = layer_norm(cells).astype(BF)
        q = split((dot(normed, fw[0]) * scale).astype(BF))
        ks, vs = key_value(normed)
        return cells, q, ks, vs

    def feature_attention(own, table):
        cells, q, ks, vs = own
        n = table.shape[0]
        more_k, more_v = key_value(layer_norm(feature_rows(table)).astype(BF))
        ks, vs = ks + more_k, vs + more_v
        mixes = []
        for f in range(quad):
            prod = jnp.concatenate([q[f] * k for k in ks], axis=0)
            s = dot(prod, spread)
            s = [s[g * n : (g + 1) * n] for g in range(len(ks))]
            top = functools.reduce(jnp.maximum, s)
            total = None
            mix = None
            for g in range(len(ks)):
                e = jnp.exp2(s[g] - top)
                t = e * vs[g].astype(F32)
                total = e if total is None else total + e
                mix = t if mix is None else mix + t
            mixes.append((mix / total).astype(BF))
        feat_out = dot(jnp.concatenate(mixes, axis=0), fw[3])
        return split((cells + feat_out).astype(BF))

    def to_mates(box, landing, stage):
        copies = {}
        for k in (2, 3, 1):
            copies[k] = pltpu.make_async_remote_copy(
                src_ref=box.at[partner(k)],
                dst_ref=landing.at[k],
                send_sem=q_send.at[stage, k],
                recv_sem=q_recv.at[stage, k],
                device_id={"rows": mate(k)},
                device_id_type=MESH,
            )
            copies[k].start()
        landing[0] = box[member]
        return copies

    loads[0].wait()
    loads[1].wait()
    own = [own_side(train_ref[p * n_half : (p + 1) * n_half]) for p in range(2)]
    moved = []
    boxes = [(outbox.at[p], inbox.at[p]) for p in range(2)] + [(t_outbox, t_inbox)]
    for p in range(2):
        swaps[p].wait()
        for f, x in enumerate(feature_attention(own[p], o_train[p * n_half : (p + 1) * n_half])):
            outbox[p, f] = pack(x)
        moved.append(to_mates(*boxes[p], p))
    loads[2].wait()
    own_test = own_side(test_ref[...])
    swaps[2].wait()
    for f, x in enumerate(feature_attention(own_test, o_test[...])):
        t_outbox[f] = pack(x)
    moved.append(to_mates(*boxes[2], 2))

    def hop(way, h, p):
        last = h == half - 1
        src = 0 if h == 0 else 2 * h - 1 + way
        dst = 2 * half - 1 if last else 1 + 2 * h + way
        return pltpu.make_async_remote_copy(
            src_ref=ring.at[src, p],
            dst_ref=ring.at[dst, p],
            send_sem=r_send.at[way, h, p],
            recv_sem=r_recv.at[way, h, p],
            device_id={"rows": left if way else right},
            device_id_type=MESH,
        )

    def pieces(way, h):
        return (way,) if h == half - 1 else (way, 1 - way)

    hops = {}
    after = []
    normed = []

    def arrive(stage):
        for k in range(1, quad):
            moved[stage][k].wait_recv()
        landing = boxes[stage][1]
        after.append(
            jnp.concatenate([unpack(landing[k]) for k in range(quad)], axis=0).astype(F32)
        )
        normed.append(layer_norm(after[stage]).astype(BF))

    for p in range(2):
        arrive(p)
        ring[0, p] = pack(normed[p])
        for way in (p, 1 - p):
            if p in pieces(way, 0):
                hops[way, 0, p] = hop(way, 0, p)
                hops[way, 0, p].start()

    loads[3].wait()
    lane_head = lax.broadcasted_iota(jnp.int32, (1, width), 1) // HD
    n_query = quad * (n_train + n_test)
    n_side = n_query // 2
    sizes = [2 * n_half, 2 * n_half, 2 * n_test]
    begins = [0, 2 * n_half, 4 * n_half]
    all_rows = [slice(0, n_query)]
    train_rows = [slice(i * n_side, i * n_side + begins[2]) for i in range(2)]
    test_rows = [slice(i * n_side + begins[2], (i + 1) * n_side) for i in range(2)]
    span = quad * n_train
    values[:, width:] = jnp.ones_like(values[:, width:])

    def ask(stage):
        q_all = (dot(normed[stage], rw[0]) * scale).astype(BF)
        n = sizes[stage]
        for h in range(heads):
            one = jnp.where(lane_head == h, q_all, jnp.zeros_like(q_all))
            for i in range(2):
                at = i * n_side + begins[stage]
                queries[h, at : at + n] = one[(1 - i) * n : (2 - i) * n]

    def take(slot, column):
        x = jnp.concatenate([unpack(ring[slot, 0]), unpack(ring[slot, 1])], axis=0)
        values[column * span : (column + 1) * span, :width] = dot(x, rw[2]).astype(BF)
        return dot(x, rw[1]).astype(BF)

    def score(key, column, rows):
        for h in range(heads):
            for r in rows:
                scores[h, r, column * span : (column + 1) * span] = dot_t(queries[h, r], key)

    def attend(h, rows, columns, carried):
        s = scores[h, rows, columns]
        top = jnp.max(s, axis=-1, keepdims=True)
        if carried is not None:
            top = jnp.maximum(top, carried[0])
        e = jnp.exp2(s - top).astype(BF)
        out = dot(e, values[columns])
        if carried is not None:
            out = out + carried[1] * jnp.exp2(carried[0] - top)
        return top, out

    ask(0)
    ask(1)
    everything = slice(0, n_query)
    if half <= 2:
        own_key = take(0, 0)
        score(own_key, 0, train_rows)
    arrive(2)
    ask(2)
    if half <= 2:
        score(own_key, 0, test_rows)
        states = [attend(h, everything, slice(0, span), None) for h in range(heads)]

    for h in range(half - 1):
        for way in range(2):
            for p in pieces(way, h + 1):
                hops[way, h, p].wait_recv()
                hops[way, h + 1, p] = hop(way, h + 1, p)
                hops[way, h + 1, p].start()
        for way in range(2):
            for p in pieces(way, h):
                if p not in pieces(way, h + 1):
                    hops[way, h, p].wait_recv()

    if half == 2:
        for slot in (1, 2):
            score(take(slot, slot), slot, all_rows)
        states = [
            attend(h, everything, slice(span, 3 * span), states[h]) for h in range(heads)
        ]

    for way in range(2):
        for p in pieces(way, half - 1):
            hops[way, half - 1, p].wait_recv()

    if half <= 2:
        last = 2 * half - 1
        last_key = take(last, last)
        columns = slice(last * span, (last + 1) * span)
    else:
        per = scores.shape[2] // span

        def step(i, states):
            for j in range(per):
                score(take(i * per + j, j), j, all_rows)
            return [attend(h, everything, slice(0, per * span), states[h]) for h in range(heads)]

        start = [
            (
                jnp.full((n_query, 1), -1e30, F32),
                jnp.zeros((n_query, values.shape[1]), F32),
            )
            for _ in range(heads)
        ]
        states = lax.fori_loop(0, groups_n // per, step, start)

    for c in loads[4:]:
        c.wait()
    returns = []
    for i, pair in enumerate(((2, 3), (0, 1))):
        rows = slice(i * n_side, (i + 1) * n_side)
        side = [tuple(x[rows] for x in states[h]) for h in range(heads)]
        if half <= 2:
            score(last_key, last, [rows])
            side = [attend(h, rows, columns, side[h]) for h in range(heads)]
        mixed = None
        for h in range(heads):
            out = side[h][1]
            part = out[:, :width] * (1.0 / out[:, width : width + 1])
            mixed = part if h == 0 else jnp.where(lane_head == h, part, mixed)
        before = [x[(1 - i) * n : (2 - i) * n] for x, n in zip(after, sizes)]
        after_row = jnp.concatenate(before, axis=0) + dot(mixed.astype(BF), rw[3])
        hidden = gelu(dot(layer_norm(after_row).astype(BF), up[...])).astype(BF)
        done = (after_row + dot_t(hidden, down[...])).astype(BF)
        for j, k in enumerate(pair):
            block = pack(
                jnp.concatenate(
                    [
                        done[b + j * (n // 2) : b + (j + 1) * (n // 2)]
                        for b, n in zip(begins, sizes)
                    ],
                    axis=0,
                )
            )
            back_out[k] = block
            if k == 0:
                c = pltpu.make_async_copy(back_out.at[0], back_in.at[member], b_send.at[0])
                c.start()
                returns.append(c)
                continue
            c = pltpu.make_async_remote_copy(
                src_ref=back_out.at[k],
                dst_ref=back_in.at[member],
                send_sem=b_send.at[k],
                recv_sem=b_recv.at[k],
                device_id={"rows": mate(k)},
                device_id_type=MESH,
            )
            c.start()
            returns.append(c)
    for c in returns:
        c.wait()
    for c in [*hops.values(), *(c for m in moved for c in m.values())]:
        c.wait_send()


def place(back_ref, train_out, test_out):
    quad = back_ref.shape[0]
    result = jnp.concatenate([unpack(back_ref[f]) for f in range(quad)], axis=1)
    n_train = train_out.shape[0]
    train_out[...] = result[:n_train]
    test_out[...] = result[n_train:]


def solution(mesh):
    rows_n = mesh.shape["rows"]
    feats_n = mesh.shape["feat"]

    def body(train, test, fw, rw, up, down):
        width = fw.shape[-1]
        quad = train.shape[1] // width
        heads = width // HD
        n_train, n_test = train.shape[0], test.shape[0]
        cell_rows = n_train + n_test
        groups_n = rows_n // quad
        half = groups_n // 2
        span = quad * n_train
        keys = min(groups_n, 4) * span
        packed = cell_rows * width // 128
        vmem = pltpu.VMEM
        dma = pltpu.SemaphoreType.DMA
        vspec = pl.BlockSpec(memory_space=pltpu.VMEM)
        aspec = pl.BlockSpec(memory_space=pl.ANY)
        back = pl.pallas_call(
            functools.partial(kernel, rows_n, feats_n),
            out_shape=jax.ShapeDtypeStruct((quad, packed, 128), BF),
            in_specs=[aspec, aspec, aspec, aspec, aspec, aspec],
            out_specs=aspec,
            scratch_shapes=[
                vmem(fw.shape, BF),
                vmem(rw.shape, BF),
                vmem(up.shape, BF),
                vmem(down.shape[::-1], BF),
                vmem(train.shape, BF),
                vmem(test.shape, BF),
                vmem(train.shape, BF),
                vmem(test.shape, BF),
                vmem((2, quad, n_train * width // 256, 128), BF),
                vmem((2, quad, n_train * width // 256, 128), BF),
                vmem((quad, n_test * width // 128, 128), BF),
                vmem((quad, n_test * width // 128, 128), BF),
                vmem((groups_n, 2, span * width // 256, 128), BF),
                vmem((heads, quad * cell_rows, keys), F32),
                vmem((keys, 256), BF),
                vmem((heads, quad * cell_rows, width), BF),
                vmem((quad, packed, 128), BF),
                dma((6,)),
                dma((3,)),
                dma((3,)),
                dma((3, quad)),
                dma((3, quad)),
                dma((2, half, 2)),
                dma((2, half, 2)),
                dma((quad,)),
                dma((quad,)),
            ],
            compiler_params=pltpu.CompilerParams(
                collective_id=0, has_side_effects=True, vmem_limit_bytes=60 * 1024 * 1024
            ),
            name="layer",
        )(train, test, fw, rw, up, down.T)
        return pl.pallas_call(
            place,
            out_shape=(
                jax.ShapeDtypeStruct(train.shape, BF),
                jax.ShapeDtypeStruct(test.shape, BF),
            ),
            in_specs=[vspec],
            out_specs=(vspec, vspec),
            name="place",
        )(back)

    return jax.shard_map(
        body,
        mesh=mesh,
        in_specs=(P("rows", "feat"), P("rows", "feat"), P(), P(), P(), P()),
        out_specs=(P("rows", "feat"), P("rows", "feat")),
        check_vma=False,
    )
```

```python
import functools

import jax
import jax.numpy as jnp
from jax import lax
from jax.experimental import pallas as pl
from jax.experimental.pallas import tpu as pltpu
from jax.sharding import PartitionSpec as P

HD = 32
EPS = 1e-05
LOG2E = 1.4426950408889634
MESH = pl.DeviceIdType.MESH
BF = jnp.bfloat16
F32 = jnp.float32


def layer_norm(x):
    centred = x - jnp.mean(x, axis=-1, keepdims=True)
    spread = jnp.mean(centred * centred, axis=-1, keepdims=True)
    return centred * lax.rsqrt(spread + EPS)


def dot(a, b):
    return jnp.dot(a, b, preferred_element_type=F32)


def dot_t(a, b):
    return lax.dot_general(a, b, (((1,), (1,)), ((), ())), preferred_element_type=F32)


def pack(x):
    n = x.shape[0]
    low = jnp.concatenate([x[: n // 2, 128:], x[n // 2 :, 128:]], axis=1)
    return jnp.concatenate([x[:, :128], low], axis=0)


def unpack(p):
    n = p.shape[0] * 2 // 3
    low = p[n:]
    high = jnp.concatenate([low[:, :64], low[:, 64:]], axis=0)
    return jnp.concatenate([p[:n], high], axis=1)


def gelu(x):
    return 0.5 * x * (1.0 + lax.erf(x * (0.5**0.5)))


def kernel(
    rows_n,
    feats_n,
    train_hbm,
    test_hbm,
    fw_hbm,
    rw_hbm,
    up_hbm,
    down_hbm,
    back_in,
    fw,
    rw,
    up,
    down,
    train_ref,
    test_ref,
    o_train,
    o_test,
    outbox,
    inbox,
    t_outbox,
    t_inbox,
    ring,
    scores,
    values,
    queries,
    back_out,
    w_sem,
    f_send,
    f_recv,
    q_send,
    q_recv,
    r_send,
    r_recv,
    b_send,
    b_recv,
):
    width = fw.shape[-1]
    quad = t_outbox.shape[0]
    heads = width // HD
    groups_n = rows_n // quad
    half = groups_n // 2
    n_train = train_ref.shape[0]
    n_test = test_ref.shape[0]
    n_half = n_train // 2
    scale = LOG2E * HD ** (-0.5)

    my_row = lax.axis_index("rows")
    my_feat = lax.axis_index("feat")
    member = lax.rem(my_row, quad)
    group = my_row // quad

    def partner(k):
        low, high = lax.rem(member, 2), member // 2
        return (1 - high if k // 2 else high) * 2 + (1 - low if k % 2 else low)

    def mate(k):
        return group * quad + partner(k)

    right = lax.rem(group + 1, groups_n) * quad + member
    left = lax.rem(group + groups_n - 1, groups_n) * quad + member
    other = lax.rem(my_feat + 1, feats_n)

    loads = [
        pltpu.make_async_copy(s, d, w_sem.at[i])
        for i, (s, d) in enumerate(
            [
                (train_hbm, train_ref),
                (fw_hbm, fw),
                (test_hbm, test_ref),
                (rw_hbm, rw),
                (up_hbm, up),
                (down_hbm, down),
            ]
        )
    ]
    for c in loads:
        c.start()

    barrier = pltpu.get_barrier_semaphore()
    pl.semaphore_signal(barrier, inc=1, device_id={"feat": other}, device_id_type=MESH)
    for k in range(1, quad):
        pl.semaphore_signal(barrier, inc=1, device_id={"rows": mate(k)}, device_id_type=MESH)
    for d in (right, left):
        pl.semaphore_signal(barrier, inc=1, device_id={"rows": d}, device_id_type=MESH)
    pl.semaphore_wait(barrier, quad + 2)

    halves = [pl.ds(p * n_half, n_half) for p in range(2)]
    swaps = [
        pltpu.make_async_remote_copy(
            src_ref=s,
            dst_ref=d,
            send_sem=f_send.at[i],
            recv_sem=f_recv.at[i],
            device_id={"feat": other},
            device_id_type=MESH,
        )
        for i, (s, d) in enumerate(
            [(train_hbm.at[r], o_train.at[r]) for r in halves] + [(test_hbm, o_test)]
        )
    ]
    for c in swaps:
        c.start()

    def feature_rows(table):
        return jnp.concatenate(
            [table[:, f * width : (f + 1) * width].astype(F32) for f in range(quad)], axis=0
        )

    def split(x):
        n = x.shape[0] // quad
        return [x[f * n : (f + 1) * n] for f in range(quad)]

    def key_value(normed):
        return split(dot(normed, fw[1]).astype(BF)), split(dot(normed, fw[2]).astype(BF))

    same = (
        lax.broadcasted_iota(jnp.int32, (width, width), 0) // HD
        == lax.broadcasted_iota(jnp.int32, (width, width), 1) // HD
    )
    spread = jnp.where(same, 1.0, 0.0).astype(BF)

    def own_side(table):
        cells = feature_rows(table)
        normed = layer_norm(cells).astype(BF)
        q = split((dot(normed, fw[0]) * scale).astype(BF))
        ks, vs = key_value(normed)
        return cells, q, ks, vs

    def feature_attention(own, table):
        cells, q, ks, vs = own
        n = table.shape[0]
        more_k, more_v = key_value(layer_norm(feature_rows(table)).astype(BF))
        ks, vs = ks + more_k, vs + more_v
        mixes = []
        for f in range(quad):
            prod = jnp.concatenate([q[f] * k for k in ks], axis=0)
            s = dot(prod, spread)
            s = [s[g * n : (g + 1) * n] for g in range(len(ks))]
            top = functools.reduce(jnp.maximum, s)
            total = None
            mix = None
            for g in range(len(ks)):
                e = jnp.exp2(s[g] - top)
                t = e * vs[g].astype(F32)
                total = e if total is None else total + e
                mix = t if mix is None else mix + t
            mixes.append((mix / total).astype(BF))
        feat_out = dot(jnp.concatenate(mixes, axis=0), fw[3])
        return split((cells + feat_out).astype(BF))

    def to_mates(box, landing, stage):
        copies = {}
        for k in (2, 3, 1):
            copies[k] = pltpu.make_async_remote_copy(
                src_ref=box.at[partner(k)],
                dst_ref=landing.at[k],
                send_sem=q_send.at[stage, k],
                recv_sem=q_recv.at[stage, k],
                device_id={"rows": mate(k)},
                device_id_type=MESH,
            )
            copies[k].start()
        landing[0] = box[member]
        return copies

    loads[0].wait()
    loads[1].wait()
    own = [own_side(train_ref[p * n_half : (p + 1) * n_half]) for p in range(2)]
    moved = []
    boxes = [(outbox.at[p], inbox.at[p]) for p in range(2)] + [(t_outbox, t_inbox)]
    for p in range(2):
        swaps[p].wait()
        for f, x in enumerate(feature_attention(own[p], o_train[p * n_half : (p + 1) * n_half])):
            outbox[p, f] = pack(x)
        moved.append(to_mates(*boxes[p], p))
    loads[2].wait()
    own_test = own_side(test_ref[...])
    swaps[2].wait()
    for f, x in enumerate(feature_attention(own_test, o_test[...])):
        t_outbox[f] = pack(x)
    moved.append(to_mates(*boxes[2], 2))

    def hop(way, h, p):
        last = h == half - 1
        src = 0 if h == 0 else 2 * h - 1 + way
        dst = 2 * half - 1 if last else 1 + 2 * h + way
        return pltpu.make_async_remote_copy(
            src_ref=ring.at[src, p],
            dst_ref=ring.at[dst, p],
            send_sem=r_send.at[way, h, p],
            recv_sem=r_recv.at[way, h, p],
            device_id={"rows": left if way else right},
            device_id_type=MESH,
        )

    def pieces(way, h):
        return (way,) if h == half - 1 else (way, 1 - way)

    hops = {}
    after = []
    normed = []

    def arrive(stage):
        for k in range(1, quad):
            moved[stage][k].wait_recv()
        landing = boxes[stage][1]
        after.append(
            jnp.concatenate([unpack(landing[k]) for k in range(quad)], axis=0).astype(F32)
        )
        normed.append(layer_norm(after[stage]).astype(BF))

    for p in range(2):
        arrive(p)
        ring[0, p] = pack(normed[p])
        for way in (p, 1 - p):
            if p in pieces(way, 0):
                hops[way, 0, p] = hop(way, 0, p)
                hops[way, 0, p].start()

    loads[3].wait()
    lane_head = lax.broadcasted_iota(jnp.int32, (1, width), 1) // HD
    n_query = quad * (n_train + n_test)
    n_side = n_query // 2
    sizes = [2 * n_half, 2 * n_half, 2 * n_test]
    begins = [0, 2 * n_half, 4 * n_half]
    all_rows = [slice(0, n_query)]
    train_rows = [slice(i * n_side, i * n_side + begins[2]) for i in range(2)]
    test_rows = [slice(i * n_side + begins[2], (i + 1) * n_side) for i in range(2)]
    span = quad * n_train
    values[:, width:] = jnp.ones_like(values[:, width:])

    def ask(stage):
        q_all = (dot(normed[stage], rw[0]) * scale).astype(BF)
        n = sizes[stage]
        for h in range(heads):
            one = jnp.where(lane_head == h, q_all, jnp.zeros_like(q_all))
            for i in range(2):
                at = i * n_side + begins[stage]
                queries[h, at : at + n] = one[(1 - i) * n : (2 - i) * n]

    def take(slot, column):
        x = jnp.concatenate([unpack(ring[slot, 0]), unpack(ring[slot, 1])], axis=0)
        values[column * span : (column + 1) * span, :width] = dot(x, rw[2]).astype(BF)
        return dot(x, rw[1]).astype(BF)

    def score(key, column, rows):
        for h in range(heads):
            for r in rows:
                scores[h, r, column * span : (column + 1) * span] = dot_t(queries[h, r], key)

    def attend(h, rows, columns, carried):
        s = scores[h, rows, columns]
        top = jnp.max(s, axis=-1, keepdims=True)
        if carried is not None:
            top = jnp.maximum(top, carried[0])
        e = jnp.exp2(s - top).astype(BF)
        out = dot(e, values[columns])
        if carried is not None:
            out = out + carried[1] * jnp.exp2(carried[0] - top)
        return top, out

    ask(0)
    ask(1)
    everything = slice(0, n_query)
    if half <= 2:
        own_key = take(0, 0)
        score(own_key, 0, train_rows)
    arrive(2)
    ask(2)
    if half <= 2:
        score(own_key, 0, test_rows)
        states = [attend(h, everything, slice(0, span), None) for h in range(heads)]

    for h in range(half - 1):
        for way in range(2):
            for p in pieces(way, h + 1):
                hops[way, h, p].wait_recv()
                hops[way, h + 1, p] = hop(way, h + 1, p)
                hops[way, h + 1, p].start()
        for way in range(2):
            for p in pieces(way, h):
                if p not in pieces(way, h + 1):
                    hops[way, h, p].wait_recv()

    if half == 2:
        for slot in (1, 2):
            score(take(slot, slot), slot, all_rows)
        states = [
            attend(h, everything, slice(span, 3 * span), states[h]) for h in range(heads)
        ]

    for way in range(2):
        for p in pieces(way, half - 1):
            hops[way, half - 1, p].wait_recv()

    if half <= 2:
        last = 2 * half - 1
        last_key = take(last, last)
        columns = slice(last * span, (last + 1) * span)
    else:
        per = scores.shape[2] // span

        def step(i, states):
            for j in range(per):
                score(take(i * per + j, j), j, all_rows)
            return [attend(h, everything, slice(0, per * span), states[h]) for h in range(heads)]

        start = [
            (
                jnp.full((n_query, 1), -1e30, F32),
                jnp.zeros((n_query, values.shape[1]), F32),
            )
            for _ in range(heads)
        ]
        states = lax.fori_loop(0, groups_n // per, step, start)

    for c in loads[4:]:
        c.wait()
    returns = []
    for i, pair in enumerate(((2, 3), (0, 1))):
        rows = slice(i * n_side, (i + 1) * n_side)
        side = [tuple(x[rows] for x in states[h]) for h in range(heads)]
        if half <= 2:
            score(last_key, last, [rows])
            side = [attend(h, rows, columns, side[h]) for h in range(heads)]
        mixed = None
        for h in range(heads):
            out = side[h][1]
            part = out[:, :width] * (1.0 / out[:, width : width + 1])
            mixed = part if h == 0 else jnp.where(lane_head == h, part, mixed)
        before = [x[(1 - i) * n : (2 - i) * n] for x, n in zip(after, sizes)]
        after_row = jnp.concatenate(before, axis=0) + dot(mixed.astype(BF), rw[3])
        hidden = gelu(dot(layer_norm(after_row).astype(BF), up[...])).astype(BF)
        done = (after_row + dot_t(hidden, down[...])).astype(BF)
        for j, k in enumerate(pair):
            block = pack(
                jnp.concatenate(
                    [
                        done[b + j * (n // 2) : b + (j + 1) * (n // 2)]
                        for b, n in zip(begins, sizes)
                    ],
                    axis=0,
                )
            )
            back_out[k] = block
            if k == 0:
                c = pltpu.make_async_copy(back_out.at[0], back_in.at[member], b_send.at[0])
                c.start()
                returns.append(c)
                continue
            c = pltpu.make_async_remote_copy(
                src_ref=back_out.at[k],
                dst_ref=back_in.at[member],
                send_sem=b_send.at[k],
                recv_sem=b_recv.at[k],
                device_id={"rows": mate(k)},
                device_id_type=MESH,
            )
            c.start()
            returns.append(c)
    for c in returns:
        c.wait()
    for c in [*hops.values(), *(c for m in moved for c in m.values())]:
        c.wait_send()


def place(back_ref, train_out, test_out):
    quad = back_ref.shape[0]
    result = jnp.concatenate([unpack(back_ref[f]) for f in range(quad)], axis=1)
    n_train = train_out.shape[0]
    train_out[...] = result[:n_train]
    test_out[...] = result[n_train:]


def solution(mesh):
    rows_n = mesh.shape["rows"]
    feats_n = mesh.shape["feat"]

    def body(train, test, fw, rw, up, down):
        width = fw.shape[-1]
        quad = train.shape[1] // width
        heads = width // HD
        n_train, n_test = train.shape[0], test.shape[0]
        cell_rows = n_train + n_test
        groups_n = rows_n // quad
        half = groups_n // 2
        span = quad * n_train
        keys = min(groups_n, 4) * span
        packed = cell_rows * width // 128
        vmem = pltpu.VMEM
        dma = pltpu.SemaphoreType.DMA
        vspec = pl.BlockSpec(memory_space=pltpu.VMEM)
        aspec = pl.BlockSpec(memory_space=pl.ANY)
        back = pl.pallas_call(
            functools.partial(kernel, rows_n, feats_n),
            out_shape=pltpu.VMEM((quad, packed, 128), BF),
            in_specs=[aspec, aspec, aspec, aspec, aspec, aspec],
            out_specs=vspec,
            scratch_shapes=[
                vmem(fw.shape, BF),
                vmem(rw.shape, BF),
                vmem(up.shape, BF),
                vmem(down.shape[::-1], BF),
                vmem(train.shape, BF),
                vmem(test.shape, BF),
                vmem(train.shape, BF),
                vmem(test.shape, BF),
                vmem((2, quad, n_train * width // 256, 128), BF),
                vmem((2, quad, n_train * width // 256, 128), BF),
                vmem((quad, n_test * width // 128, 128), BF),
                vmem((quad, n_test * width // 128, 128), BF),
                vmem((groups_n, 2, span * width // 256, 128), BF),
                vmem((heads, quad * cell_rows, keys), F32),
                vmem((keys, 256), BF),
                vmem((heads, quad * cell_rows, width), BF),
                vmem((quad, packed, 128), BF),
                dma((6,)),
                dma((3,)),
                dma((3,)),
                dma((3, quad)),
                dma((3, quad)),
                dma((2, half, 2)),
                dma((2, half, 2)),
                dma((quad,)),
                dma((quad,)),
            ],
            compiler_params=pltpu.CompilerParams(
                collective_id=0, has_side_effects=True, vmem_limit_bytes=60 * 1024 * 1024
            ),
            name="layer",
        )(train, test, fw, rw, up, down.T)
        return pl.pallas_call(
            place,
            out_shape=(
                jax.ShapeDtypeStruct(train.shape, BF),
                jax.ShapeDtypeStruct(test.shape, BF),
            ),
            in_specs=[vspec],
            out_specs=(vspec, vspec),
            name="place",
        )(pltpu.with_memory_space_constraint(back, pltpu.VMEM))

    return jax.shard_map(
        body,
        mesh=mesh,
        in_specs=(P("rows", "feat"), P("rows", "feat"), P(), P(), P(), P()),
        out_specs=(P("rows", "feat"), P("rows", "feat")),
        check_vma=False,
    )
```
